512 devices in a mesh: groups: 2 (over y), nodes: 32 (over z), heads: 4 (over x), sub: 2 (over core).
Axes of the slice: x: 4, y: 2, z: 32, core: 2. Of those that a mesh axis runs over, the one named last changes fastest.
The devices are a block of a 4x8x32 slice.
Arguments:
- queries: bfloat16 [32768, 512], P(('groups', 'nodes', 'sub'), 'heads'), parts along dimension 0, may hold values from -60 to 60
- key_vectors: bfloat16 [32768, 512], P(('groups', 'nodes', 'sub'), 'heads'), parts along dimension 0, may hold values from -20 to 20
- value_vectors: bfloat16 [32768, 512], P(('groups', 'nodes', 'sub'), 'heads'), parts along dimension 0, may hold values from -6 to 6
- cotangent: bfloat16 [32768, 512], P(('groups', 'nodes', 'sub'), 'heads'), parts along dimension 0, may hold values from -6 to 6
- out_weight: bfloat16 [512, 512], P('heads'), may hold values from -0.25 to 0.25
- neighbours: int32 [256, 16], P('groups'), parts along dimension 0, may hold values from 0 to 127, as said below
- entry_mask: int32 [256, 16], P('groups'), parts along dimension 0, may hold values from 0 to 1, as said below
- live_counts: int32 [128], P('groups'), parts along dimension 0, may hold values from 1 to 2, as said below
- tile_slot: int32 [256], P('groups'), parts along dimension 0, may hold values from 0 to 127, as said below
Outputs:
- query_grad: bfloat16 [32768, 512], P(('groups', 'nodes', 'sub'), 'heads'), parts along dimension 0
- key_grad: bfloat16 [32768, 512], P(('groups', 'nodes', 'sub'), 'heads'), parts along dimension 0
- value_grad: bfloat16 [32768, 512], P(('groups', 'nodes', 'sub'), 'heads'), parts along dimension 0
- weight_grad: float32 [1024, 512], P(('groups', 'heads')), parts along dimension 0
The draws below stay inside these ranges and needn't reach their ends.
There are 2 independent parts, one for each index of `groups`. The reference program is written for one: setup_inputs(seed, part) draws one part's arguments, and reference() takes and returns one part's arrays. A program takes and returns all parts, laid end to end along the dimension named above; an argument that names none is the same for every part. Nothing has to cross between parts.
Inputs may be any that keep to these rules, and one draw needn't show every extreme that they name: `neighbours`: row r lists graph tiles for the query tile in slot r. Entry 0 is that tile itself; entries 1 to 7 name live tiles of the same shard; entries 8 to 15 name live tiles of the shards next to it (shard index one lower or one higher, none past either end). Entries may repeat. Over all rows of one shard, the entries name at most one distinct tile of each adjacent shard, and in every draw some shard names exactly one tile of an adjacent shard. `entry_mask`: entry 0 of every row is 1. The live tiles of shard s are its slots s * 2 to s * 2 + live_counts[s] - 1; at least one shard is full. `tile_slot`: the graph tiles g with g // 2 = s are held in the slots of shard s, each slot once.
All inputs are finite; a program needn't handle non-finite values.
Results may differ from the reference program's by a relative error of at most 0.025.
Values may be sent and summed in bfloat16 or wider, within the bound.
No kernel may reach another device: no remote copies, remote signals or barrier semaphores. Data moves between devices by JAX's collectives and lax.ppermute only.
A program may use at most 64 MiB of HBM per device.

```python
import jax
import jax.numpy as jnp
from jax import lax

D = 512
HEADS = 8
HD = 64
TILE = 128
TILES_DEV = 2
DEG_IN = 8
DEG_OUT = 8
DEG = 16
HALO_CAP = 1
SHARDS = 64
TILES = 128
NODES = 16384


def query_key_pair(base_key):
    folded = jax.random.fold_in(base_key, 101)
    query_key, vector_key = jax.random.split(folded, 2)
    key_base = jnp.clip(jax.random.normal(vector_key, (NODES, D), jnp.float32), -4.0, 4.0) * 1.25
    query_base = jnp.clip(jax.random.normal(query_key, (NODES, D), jnp.float32), -4.0, 4.0) * 1.25
    return (query_base, key_base)


def tile_graph(base_key):
    folded = jax.random.fold_in(base_key, 202)
    count_key, full_key, perm_key, inner_key, side_key, pick_key, order_key, mask_key = jax.random.split(folded, 8)
    shard_range = jnp.arange(SHARDS, dtype=jnp.int32)
    tile_range = jnp.arange(TILES_DEV, dtype=jnp.int32)
    lowest = max(1, TILES_DEV // 4)
    counts = jax.random.randint(count_key, (SHARDS,), lowest, TILES_DEV + 1)
    full_shard = jax.random.randint(full_key, (), 0, SHARDS)
    counts = jnp.where(shard_range == full_shard, TILES_DEV, counts).astype(jnp.int32)
    orders = jax.random.randint(perm_key, (SHARDS, TILES_DEV), 0, 1 << 16) * TILES_DEV + tile_range[None, :]
    local_of_graph = jnp.argsort(orders, axis=1).astype(jnp.int32)
    tile_slot = (shard_range[:, None] * TILES_DEV + local_of_graph).reshape(TILES).astype(jnp.int32)
    graph_of_local = jnp.argsort(local_of_graph, axis=1).astype(jnp.int32)
    graph_of_slot = (shard_range[:, None] * TILES_DEV + graph_of_local).reshape(TILES)
    own_entry = graph_of_slot.reshape(SHARDS, TILES_DEV, 1)
    inner_local = jax.random.randint(inner_key, (SHARDS, TILES_DEV, DEG_IN - 1), 0, 1 << 20) % counts[:, None, None]
    inner_entries = jnp.take(graph_of_slot, shard_range[:, None, None] * TILES_DEV + inner_local)
    below_count = jnp.take(counts, jnp.maximum(shard_range - 1, 0))
    above_count = jnp.take(counts, jnp.minimum(shard_range + 1, SHARDS - 1))
    side_counts = jnp.stack([below_count, above_count], axis=1)
    ranking = jax.random.randint(order_key, (SHARDS, 2, TILES_DEV), 0, 1 << 16) * TILES_DEV + tile_range[None, None, :]
    ranking = ranking + (tile_range[None, None, :] >= side_counts[:, :, None]).astype(jnp.int32) * (1 << 24)
    chosen_sets = jnp.argsort(ranking, axis=2)[:, :, :HALO_CAP].astype(jnp.int32)
    set_sizes = jnp.minimum(side_counts, HALO_CAP)
    flat_pick = jnp.arange(TILES_DEV * DEG_OUT, dtype=jnp.int32).reshape(TILES_DEV, DEG_OUT)
    covering = flat_pick < 2 * HALO_CAP
    random_side = jax.random.randint(side_key, (SHARDS, TILES_DEV, DEG_OUT), 0, 2)
    side_bit = jnp.where(covering[None], flat_pick[None] % 2, random_side)
    side_bit = jnp.where(shard_range[:, None, None] == 0, 1, side_bit)
    side_bit = jnp.where(shard_range[:, None, None] == SHARDS - 1, 0, side_bit)
    size_here = jnp.where(side_bit == 1, set_sizes[:, 1][:, None, None], set_sizes[:, 0][:, None, None])
    random_pick = jax.random.randint(pick_key, (SHARDS, TILES_DEV, DEG_OUT), 0, 1 << 20)
    element = jnp.where(covering[None], flat_pick[None] // 2, random_pick) % size_here
    set_index = (shard_range[:, None, None] * 2 + side_bit) * HALO_CAP + element
    local_pick = jnp.take(chosen_sets.reshape(-1), set_index)
    adjacent = shard_range[:, None, None] + 2 * side_bit - 1
    outer_entries = jnp.take(graph_of_slot, adjacent * TILES_DEV + local_pick)
    neighbours = jnp.concatenate([own_entry, inner_entries, outer_entries], axis=2).reshape(TILES, DEG).astype(jnp.int32)
    entry_mask = (jax.random.randint(mask_key, (TILES, DEG), 0, 4) < 3).astype(jnp.int32)
    entry_mask = entry_mask.at[:, 0].set(1)
    return (neighbours, entry_mask, counts, tile_slot)


def draw_queries(key, part):
    return query_key_pair(key)[0].astype(jnp.bfloat16)


def draw_key_vectors(key, part):
    return query_key_pair(key)[1].astype(jnp.bfloat16)


def draw_neighbours(key, part):
    return tile_graph(key)[0]


def draw_entry_mask(key, part):
    return tile_graph(key)[1]


def draw_live_counts(key, part):
    return tile_graph(key)[2]


def draw_tile_slot(key, part):
    return tile_graph(key)[3]


def level_of(rng, shape, cuts, least, largest):
    level = 1.0
    for axis_at, blocks in cuts:
        heights = jax.random.uniform(jax.random.fold_in(jax.random.fold_in(rng, 6), axis_at), (blocks,), jnp.float32, least / len(cuts), largest / len(cuts))
        level = level * jnp.repeat(jnp.exp(heights), shape[axis_at] // blocks).reshape((-1,) + (1,) * (len(shape) - 1 - axis_at))
    return level


def gaussian(own_key, dims, deviation, most, cuts=(), kind=jnp.bfloat16):
    gain = level_of(own_key, dims, cuts, -0.22, 0.18) if cuts else 1.0
    drawn = jax.random.normal(own_key, dims, jnp.float32) * deviation * gain
    return jnp.minimum(jnp.maximum(drawn, -most), most).astype(kind)


def setup_inputs(seed: int = 0, part: int = 0) -> dict:
    keys = jax.random.split(jax.random.key(seed), 10)
    part_keys = jax.random.split(jax.random.fold_in(keys[9], part), 10)
    return {
        "queries": draw_queries(jax.random.fold_in(jax.random.fold_in(keys[9], part), 71), part),
        "key_vectors": draw_key_vectors(jax.random.fold_in(jax.random.fold_in(keys[9], part), 71), part),
        "value_vectors": gaussian(part_keys[2], (NODES, D), 1.0, 6.0, ((0, 64), (1, 4))),
        "cotangent": gaussian(part_keys[3], (NODES, D), 1.0, 6.0, ((0, 64), (1, 4))),
        "out_weight": gaussian(keys[4], (D, D), D ** -0.5, 0.25, ((0, 4),)),
        "neighbours": draw_neighbours(jax.random.fold_in(jax.random.fold_in(keys[9], part), 71), part),
        "entry_mask": draw_entry_mask(jax.random.fold_in(jax.random.fold_in(keys[9], part), 71), part),
        "live_counts": draw_live_counts(jax.random.fold_in(jax.random.fold_in(keys[9], part), 71), part),
        "tile_slot": draw_tile_slot(jax.random.fold_in(jax.random.fold_in(keys[9], part), 71), part),
    }


def tile_terms(query_heads, grad_heads, key_heads, value_heads, usable, living):
    head_size = query_heads.shape[-1]
    scaling = head_size ** -0.5
    scores = jnp.einsum("athd,aeshd->ahtes", query_heads, key_heads) * scaling
    visible = usable[:, None, None, :, None]
    scores = jnp.where(visible, scores, -1e30)
    topmost = jnp.max(scores, axis=(3, 4), keepdims=True)
    expanded = jnp.where(visible, jnp.exp(scores - topmost), 0.0)
    denominator = jnp.sum(expanded, axis=(3, 4), keepdims=True)
    denominator = jnp.where(living[:, None, None, None, None], denominator, 1.0)
    weights = expanded / denominator
    rounded = lax.optimization_barrier(weights.astype(jnp.bfloat16)).astype(jnp.float32)
    attended = jnp.einsum("ahtes,aeshd->athd", rounded, value_heads).astype(jnp.bfloat16)
    row_delta = jnp.sum(grad_heads * attended.astype(jnp.float32), axis=3)
    grad_scores = jnp.einsum("athd,aeshd->ahtes", grad_heads, value_heads)
    score_grad = weights * (grad_scores - jnp.transpose(row_delta, (0, 2, 1))[:, :, :, None, None]) * scaling
    score_half = lax.optimization_barrier(score_grad.astype(jnp.bfloat16)).astype(jnp.float32)
    query_part = jnp.einsum("ahtes,aeshd->athd", score_half, key_heads)
    key_part = jnp.einsum("ahtes,athd->aeshd", score_half, query_heads)
    value_part = jnp.einsum("ahtes,athd->aeshd", rounded, grad_heads)
    return query_part, attended, key_part, value_part


def reference(queries, key_vectors, value_vectors, cotangent, out_weight, neighbours, entry_mask, live_counts, tile_slot):
    out_grad = jnp.dot(cotangent, out_weight.T, preferred_element_type=jnp.float32).astype(jnp.bfloat16)
    tile_range = jnp.arange(TILES, dtype=jnp.int32)
    living = (tile_range % TILES_DEV) < jnp.take(live_counts, tile_range // TILES_DEV)
    usable = (entry_mask == 1) & living[:, None]
    key_slot = jnp.take(tile_slot, neighbours).astype(jnp.int32)
    tile_shape = (TILES, TILE, HEADS, HD)
    query_tiles = queries.astype(jnp.float32).reshape(tile_shape)
    key_tiles = key_vectors.astype(jnp.float32).reshape(tile_shape)
    value_tiles = value_vectors.astype(jnp.float32).reshape(tile_shape)
    grad_tiles = out_grad.astype(jnp.float32).reshape(tile_shape)
    pair_tiles = 2

    def advance(running, block_number):
        key_total, value_total = running
        first_tile = block_number * pair_tiles
        entries = lax.dynamic_slice_in_dim(key_slot, first_tile, pair_tiles, 0)
        query_part, attended, key_part, value_part = tile_terms(
            lax.dynamic_slice_in_dim(query_tiles, first_tile, pair_tiles, 0),
            lax.dynamic_slice_in_dim(grad_tiles, first_tile, pair_tiles, 0),
            jnp.take(key_tiles, entries, axis=0),
            jnp.take(value_tiles, entries, axis=0),
            lax.dynamic_slice_in_dim(usable, first_tile, pair_tiles, 0),
            lax.dynamic_slice_in_dim(living, first_tile, pair_tiles, 0))
        flat_entries = entries.reshape(-1)
        key_total = key_total.at[flat_entries].add(key_part.reshape(pair_tiles * DEG, TILE, HEADS, HD))
        value_total = value_total.at[flat_entries].add(value_part.reshape(pair_tiles * DEG, TILE, HEADS, HD))
        return (key_total, value_total), (query_part, attended)

    zero_tiles = jnp.zeros(tile_shape, jnp.float32)
    totals, outputs = lax.scan(advance, (zero_tiles, zero_tiles), jnp.arange(TILES // pair_tiles, dtype=jnp.int32))
    query_grad = outputs[0].reshape(NODES, D).astype(jnp.bfloat16)
    attended = outputs[1].reshape(NODES, D)
    key_grad = totals[0].reshape(NODES, D).astype(jnp.bfloat16)
    value_grad = totals[1].reshape(NODES, D).astype(jnp.bfloat16)
    weight_grad = jnp.dot(attended.T, cotangent, preferred_element_type=jnp.float32) * NODES ** -0.5
    return query_grad, key_grad, value_grad, weight_grad
```

```python
import functools

import jax
import jax.numpy as jnp
from jax import lax
from jax.experimental import pallas as pl
from jax.experimental.pallas import tpu as pltpu
from jax.sharding import PartitionSpec as P

HD = 64
TILE = 128
LANES = 128
NODE_AXES = ("far", "near", "sub")
BLOCK_AXES = ("near", "sub")
NEAR = 4
f32 = jnp.float32
bf16 = jnp.bfloat16


def vmem(count):
    return [pl.BlockSpec(memory_space=pltpu.VMEM)] * count


def dot(a, b, dims):
    return lax.dot_general(a, b, (dims, ((), ())), preferred_element_type=f32)


def lane_total(values):
    return jnp.sum(values, axis=1, keepdims=True)


def select_kernel(lists, masks, slots, lives, keys, values, to_upper, to_lower, table):
    entries, graph_slots = lists.shape
    tiles = keys.shape[0] // TILE
    shard = (lax.axis_index("far") * lax.axis_size("near") + lax.axis_index("near")) * lax.axis_size("sub") + lax.axis_index("sub")
    names = lists[...]
    own_slot = jnp.broadcast_to(slots[...], names.shape)
    pointed = jnp.take_along_axis(own_slot, names, axis=1)
    lane = lax.broadcasted_iota(jnp.int32, names.shape, 1)
    row_shard = lane // tiles
    local = pointed % tiles
    offset = pointed // tiles - row_shard
    live_lane = lax.broadcasted_iota(jnp.int32, lives.shape, 1)
    live = lane_total(jnp.where(live_lane == shard, lives[...], 0).astype(f32))
    usable = (masks[...] == 1).astype(f32)

    def named(reader, side):
        hit = (row_shard == reader) & (offset == side)
        found = jnp.max(jnp.where(hit, local, 0), axis=1, keepdims=True).astype(f32)
        return jnp.max(found, axis=0, keepdims=True)

    up_pick = named(shard + 1, -1)
    down_pick = named(shard - 1, 1)

    def pick(source, which):
        out = source[0:TILE, :]
        wide = jnp.broadcast_to(which, (TILE, LANES))
        for t in range(1, tiles):
            out = jnp.where(wide == t, source[t * TILE : (t + 1) * TILE, :].astype(f32), out.astype(f32)).astype(bf16)
        return out

    to_upper[0] = pick(keys, up_pick)
    to_upper[1] = pick(values, up_pick)
    to_lower[0] = pick(keys, down_pick)
    to_lower[1] = pick(values, down_pick)
    rows = []
    for t in range(tiles):
        here = lane == shard * tiles + t
        for b in range(tiles + 2):
            if b < tiles:
                hit = (offset == 0) & (local == b)
            else:
                hit = offset == (-1 if b == tiles else 1)
            count = jnp.sum(jnp.where(here & hit, usable, 0.0), axis=0, keepdims=True)
            count = lane_total(count)
            rows.append(jnp.where(live > t, count, 0.0))
    rows += [up_pick, down_pick]
    for r, value in enumerate(rows):
        table[r : r + 1, :] = jnp.broadcast_to(value, (1, LANES))


def head_rows(array, tiles, heads):
    feature = lax.broadcasted_iota(jnp.int32, (TILE, array.shape[1]), 1) // HD
    out = []
    for t in range(tiles):
        part = array[t * TILE : (t + 1) * TILE, :]
        for h in range(heads):
            out.append(jnp.where(feature == h, part, jnp.zeros_like(part)))
    return jnp.concatenate(out, axis=0)


def heads_merged(array, tiles, heads):
    feature = lax.broadcasted_iota(jnp.int32, (TILE, array.shape[1]), 1) // HD
    out = []
    for t in range(tiles):
        part = array[t * heads * TILE : (t * heads + 1) * TILE, :]
        for h in range(1, heads):
            row = (t * heads + h) * TILE
            part = jnp.where(feature == h, array[row : row + TILE, :], part)
        out.append(part)
    return jnp.concatenate(out, axis=0)


def forward_kernel(queries, keys, values, lower, upper, table, cots, attended, weights, product, *, heads):
    tiles = queries.shape[0] // TILE
    banks = tiles + 2
    bank_k = jnp.concatenate([keys[...], lower[0], upper[0]], axis=0)
    bank_v = jnp.concatenate([values[...], lower[1], upper[1]], axis=0)
    rows = head_rows(queries[...], tiles, heads)
    scores = dot(rows, bank_k, ((1,), (1,))) * (HD**-0.5)
    span = heads * TILE
    halves = []
    for t in range(tiles):
        blocks, counts = [], []
        for b in range(banks):
            count = table[t * banks + b : t * banks + b + 1, :]
            block = scores[t * span : (t + 1) * span, b * TILE : (b + 1) * TILE]
            blocks.append(jnp.where(count > 0.0, block, -1e30))
            counts.append(count)
        top = functools.reduce(jnp.maximum, blocks)
        top = jnp.max(top, axis=1, keepdims=True)
        blocks = [jnp.exp(block - top) * count for block, count in zip(blocks, counts)]
        total = lane_total(functools.reduce(jnp.add, blocks))
        inverse = 1.0 / jnp.where(total > 0.0, total, 1.0)
        halves.append(jnp.concatenate([block * inverse for block in blocks], axis=1).astype(bf16))
    weight = jnp.concatenate(halves, axis=0)
    weights[...] = weight
    result = heads_merged(dot(weight, bank_v, ((1,), (0,))), tiles, heads).astype(bf16)
    attended[...] = result
    parts = cots.shape[0]
    terms = [dot(result, cots[j], ((0,), (0,))) for j in range(parts)]
    share, rows_each = product.shape[0] // parts, product.shape[1]
    for j, term in enumerate(terms):
        for k in range(share):
            product[j * share + k] = term[k * rows_each : (k + 1) * rows_each, :].astype(product.dtype)


def backward_kernel(queries, keys, values, lower, upper, weights, attended, cots, out_weight, query_grad, key_part, value_part, to_lower, to_upper, *, heads):
    tiles = queries.shape[0] // TILE
    scale = HD**-0.5
    own = keys.shape[0]
    total = None
    for j in range(cots.shape[0]):
        term = dot(cots[j], out_weight[:, j * LANES : (j + 1) * LANES], ((1,), (1,)))
        total = term if total is None else total + term
    out_grad = total.astype(bf16)
    bank_k = jnp.concatenate([keys[...], lower[0], upper[0]], axis=0)
    bank_v = jnp.concatenate([values[...], lower[1], upper[1]], axis=0)
    rows = head_rows(queries[...], tiles, heads)
    grads = head_rows(out_grad, tiles, heads)
    mixed = head_rows((out_grad.astype(f32) * attended[...].astype(f32)), tiles, heads)
    delta = lane_total(mixed)
    weight = weights[...]
    grad_scores = dot(grads, bank_v, ((1,), (1,)))
    score_grad = (weight.astype(f32) * (grad_scores - delta) * scale).astype(bf16)
    query_grad[...] = heads_merged(dot(score_grad, bank_k, ((1,), (0,))), tiles, heads).astype(bf16)
    key_all = dot(score_grad, rows, ((0,), (0,)))
    value_all = dot(weight, grads, ((0,), (0,)))
    key_part[...] = key_all[0:own, :]
    value_part[...] = value_all[0:own, :]
    to_lower[0] = key_all[own : own + TILE, :].astype(bf16)
    to_lower[1] = value_all[own : own + TILE, :].astype(bf16)
    to_upper[0] = key_all[own + TILE :, :].astype(bf16)
    to_upper[1] = value_all[own + TILE :, :].astype(bf16)


def combine_kernel(key_part, value_part, from_lower, from_upper, table, key_grad, value_grad):
    tiles = key_part.shape[0] // TILE
    at = tiles * (tiles + 2)
    up_pick = table[at : at + 1, :]
    down_pick = table[at + 1 : at + 2, :]
    for k, (part, out) in enumerate(((key_part, key_grad), (value_part, value_grad))):
        for t in range(tiles):
            value = part[t * TILE : (t + 1) * TILE, :]
            value = value + jnp.where(up_pick == t, from_upper[k].astype(f32), 0.0)
            value = value + jnp.where(down_pick == t, from_lower[k].astype(f32), 0.0)
            out[t * TILE : (t + 1) * TILE, :] = value.astype(bf16)


def sum_kernel(parts, total):
    value = parts[0].astype(f32)
    for j in range(1, parts.shape[0]):
        value = value + parts[j].astype(f32)
    value = value.astype(total.dtype)
    if len(total.shape) == len(value.shape):
        total[...] = value
    else:
        for j in range(total.shape[0]):
            total[j] = value


def place_kernel(parts, out, *, scale):
    count, rows_each = parts.shape[0], parts.shape[1]
    share = out.shape[0] // rows_each
    for q in range(count):
        j, k = q // share, q % share
        out[k * rows_each : (k + 1) * rows_each, j * LANES : (j + 1) * LANES] = parts[q].astype(f32) * scale


def call(kernel, out_shapes, inputs, name):
    return pl.pallas_call(
        kernel,
        out_shape=tuple(out_shapes),
        in_specs=vmem(len(inputs)),
        out_specs=tuple(vmem(len(out_shapes))),
        name=name,
    )(*inputs)


def near(array):
    return pltpu.with_memory_space_constraint(array, pltpu.VMEM)


def shape(dims, kind):
    return pltpu.VMEM(tuple(dims), kind)


def final(dims, kind):
    return jax.ShapeDtypeStruct(tuple(dims), kind)


def passed_along(value, axis, steps):
    count = lax.axis_size(axis)
    first, last = (max(0, -steps), min(count, count - steps))
    return lax.ppermute(value, axis, [(source, source + steps) for source in range(first, last)])


def block_total(product):
    parts = lax.all_to_all(product, BLOCK_AXES, 0, 0)
    kind = shape((lax.axis_size("far"),) + product.shape[1:], bf16)
    return call(sum_kernel, [kind], [near(parts)], "sum_block")[0]


def spread_total(parts, block, node_count, width):
    rows_each = parts.shape[1]
    (spread,) = call(sum_kernel, [shape((block, rows_each, LANES), bf16)], [near(parts)], "sum_far")
    parts = lax.all_to_all(spread, BLOCK_AXES, 0, 0)
    (out,) = call(
        functools.partial(place_kernel, scale=node_count**-0.5),
        [final((width, block * rows_each // width * LANES), f32)],
        [near(parts)],
        "place",
    )
    return out


def on_device(queries, key_vectors, value_vectors, cotangent, out_weight, neighbours, entry_mask, live_counts, tile_slot):
    row_count, width = queries.shape
    tiles = row_count // TILE
    heads = width // HD
    banks = tiles + 2
    columns = lax.axis_size("heads")
    block = lax.axis_size(BLOCK_AXES)
    table_rows = tiles * banks + 2
    table_rows += -table_rows % 8
    side = shape((2, TILE, width), bf16)
    to_upper, to_lower, table = call(
        select_kernel,
        [side, side, shape((table_rows, LANES), f32)],
        [neighbours.T, entry_mask.T, tile_slot[None, :], live_counts[None, :], key_vectors, value_vectors],
        "select_tiles",
    )
    cots = lax.all_to_all(jnp.broadcast_to(cotangent[None], (columns, row_count, width)), "heads", 0, 0)
    lower = passed_along(to_upper, NODE_AXES, 1)
    upper = passed_along(to_lower, NODE_AXES, -1)
    stacked = tiles * heads * TILE
    attended, weights, product = call(
        functools.partial(forward_kernel, heads=heads),
        [shape((row_count, width), bf16), shape((stacked, banks * TILE), bf16), shape((block, columns * width // block, LANES), bf16)],
        [queries, key_vectors, value_vectors, *map(near, (lower, upper, table, cots))],
        "attend",
    )
    own = block_total(product)
    parts = lax.all_to_all(own, "far", 0, 0)
    attended, weights, _ = lax.optimization_barrier((attended, weights, own))
    query_grad, key_part, value_part, down, up = call(
        functools.partial(backward_kernel, heads=heads),
        [final((row_count, width), bf16), shape((row_count, width), f32), shape((row_count, width), f32), side, side],
        [queries, key_vectors, value_vectors, *map(near, (lower, upper, weights, attended, cots)), out_weight],
        "attend_grad",
    )
    from_upper = passed_along(down, NODE_AXES, -1)
    from_lower = passed_along(up, NODE_AXES, 1)
    key_grad, value_grad = call(
        combine_kernel,
        [final((row_count, width), bf16)] * 2,
        [near(x) for x in (key_part, value_part, from_lower, from_upper, table)],
        "combine",
    )
    parts, query_grad, key_grad, value_grad = lax.optimization_barrier((parts, query_grad, key_grad, value_grad))
    weight_grad = spread_total(parts, block, row_count * lax.axis_size(NODE_AXES), width)
    return (query_grad, key_grad, value_grad, weight_grad)


def solution(mesh):
    sizes = mesh.shape
    far = sizes["nodes"] // NEAR
    split = jax.sharding.Mesh(
        mesh.devices.reshape(sizes["groups"], far, NEAR, sizes["heads"], sizes["sub"]),
        ("groups", "far", "near", "heads", "sub"),
    )
    rows = P(("groups",) + NODE_AXES, "heads")
    return jax.shard_map(
        on_device,
        mesh=split,
        in_specs=(rows, rows, rows, rows, P("heads", None), P("groups", None), P("groups", None), P("groups"), P("groups")),
        out_specs=(rows, rows, rows, P(("groups", "heads"), None)),
        check_vma=False,
    )
```

```python
import functools

import jax
import jax.numpy as jnp
from jax import lax
from jax.experimental import pallas as pl
from jax.experimental.pallas import tpu as pltpu
from jax.sharding import PartitionSpec as P

HD = 64
TILE = 128
LANES = 128
NODE_AXES = ("far", "near", "sub")
BLOCK_AXES = ("near", "sub")
NEAR = 4
f32 = jnp.float32
bf16 = jnp.bfloat16


def vmem(count):
    return [pl.BlockSpec(memory_space=pltpu.VMEM)] * count


def dot(a, b, dims):
    return lax.dot_general(a, b, (dims, ((), ())), preferred_element_type=f32)


def lane_total(values):
    return jnp.sum(values, axis=1, keepdims=True)


def select_kernel(lists, masks, slots, lives, keys, values, to_pair, to_cross, table):
    tiles = keys.shape[0] // TILE
    core = lax.axis_index("sub")
    shard = (lax.axis_index("far") * lax.axis_size("near") + lax.axis_index("near")) * lax.axis_size("sub") + core
    toward_pair = 1 - 2 * core
    names = lists[...]
    pointed = jnp.take_along_axis(jnp.broadcast_to(slots[...], names.shape), names, axis=1)
    lane = lax.broadcasted_iota(jnp.int32, names.shape, 1)
    row_shard = lane // tiles
    local = pointed % tiles
    offset = pointed // tiles - row_shard
    live_lane = lax.broadcasted_iota(jnp.int32, lives.shape, 1)
    live = lane_total(jnp.where(live_lane == shard, lives[...], 0).astype(f32))
    usable = (masks[...] == 1).astype(f32)

    def named(side):
        hit = (row_shard == shard + side) & (offset == -side)
        found = jnp.max(jnp.where(hit, local, 0), axis=1, keepdims=True).astype(f32)
        return jnp.max(found, axis=0, keepdims=True)

    def pick(source, which):
        out = source[0:TILE, :]
        wide = jnp.broadcast_to(which, (TILE, LANES))
        for t in range(1, tiles):
            out = jnp.where(wide == t, source[t * TILE : (t + 1) * TILE, :].astype(f32), out.astype(f32)).astype(bf16)
        return out

    pair_pick = named(toward_pair)
    cross_pick = named(-toward_pair)
    for out, which in ((to_pair, pair_pick), (to_cross, cross_pick)):
        out[0] = pick(keys, which)
        out[1] = pick(values, which)
    rows = []
    for t in range(tiles):
        here = lane == shard * tiles + t
        hits = [(offset == 0) & (local == b) for b in range(tiles)]
        hits += [offset == toward_pair, offset == -toward_pair]
        for hit in hits:
            count = lane_total(jnp.sum(jnp.where(here & hit, usable, 0.0), axis=0, keepdims=True))
            rows.append(jnp.where(live > t, count, 0.0))
    rows += [pair_pick, cross_pick]
    for r, value in enumerate(rows):
        table[r : r + 1, :] = jnp.broadcast_to(value, (1, LANES))


def head_rows(array, tiles, heads):
    feature = lax.broadcasted_iota(jnp.int32, (TILE, array.shape[1]), 1) // HD
    out = []
    for t in range(tiles):
        part = array[t * TILE : (t + 1) * TILE, :]
        for h in range(heads):
            out.append(jnp.where(feature == h, part, jnp.zeros_like(part)))
    return jnp.concatenate(out, axis=0)


def heads_merged(array, tiles, heads):
    feature = lax.broadcasted_iota(jnp.int32, (TILE, array.shape[1]), 1) // HD
    out = []
    for t in range(tiles):
        part = array[t * heads * TILE : (t * heads + 1) * TILE, :]
        for h in range(1, heads):
            row = (t * heads + h) * TILE
            part = jnp.where(feature == h, array[row : row + TILE, :], part)
        out.append(part)
    return jnp.concatenate(out, axis=0)


def forward_kernel(queries, keys, values, pair, cross, table, *rest, heads):
    cots, (attended, weights, product) = rest[:-3], rest[-3:]
    tiles = queries.shape[0] // TILE
    banks = tiles + 2
    bank_k = jnp.concatenate([keys[...], pair[0], cross[0]], axis=0)
    bank_v = jnp.concatenate([values[...], pair[1], cross[1]], axis=0)
    rows = head_rows(queries[...], tiles, heads)
    scores = dot(rows, bank_k, ((1,), (1,))) * (HD**-0.5)
    span = heads * TILE
    halves = []
    for t in range(tiles):
        blocks, counts = [], []
        for b in range(banks):
            count = table[t * banks + b : t * banks + b + 1, :]
            block = scores[t * span : (t + 1) * span, b * TILE : (b + 1) * TILE]
            blocks.append(jnp.where(count > 0.0, block, -1e30))
            counts.append(count)
        top = functools.reduce(jnp.maximum, blocks)
        top = jnp.max(top, axis=1, keepdims=True)
        blocks = [jnp.exp(block - top) * count for block, count in zip(blocks, counts)]
        total = lane_total(functools.reduce(jnp.add, blocks))
        inverse = 1.0 / jnp.where(total > 0.0, total, 1.0)
        halves.append(jnp.concatenate([block * inverse for block in blocks], axis=1).astype(bf16))
    weight = jnp.concatenate(halves, axis=0)
    weights[...] = weight
    result = heads_merged(dot(weight, bank_v, ((1,), (0,))), tiles, heads).astype(bf16)
    attended[...] = result
    parts = len(cots)
    terms = [dot(result, c[...], ((0,), (0,))) for c in cots]
    share, rows_each = product.shape[0] // parts, product.shape[1]
    for j, term in enumerate(terms):
        for k in range(share):
            product[j * share + k] = term[k * rows_each : (k + 1) * rows_each, :].astype(product.dtype)


def backward_kernel(queries, keys, values, pair, cross, weights, attended, out_weight, *rest, heads):
    cots, (query_grad, key_part, value_part, to_pair, to_cross) = rest[:-5], rest[-5:]
    column = lax.axis_index("heads")
    tiles = queries.shape[0] // TILE
    scale = HD**-0.5
    own = keys.shape[0]
    total = None
    for k, c in enumerate(cots):
        start = pl.multiple_of((column ^ k) * LANES, LANES)
        term = dot(c[...], out_weight[:, pl.ds(start, LANES)], ((1,), (1,)))
        total = term if total is None else total + term
    out_grad = total.astype(bf16)
    bank_k = jnp.concatenate([keys[...], pair[0], cross[0]], axis=0)
    bank_v = jnp.concatenate([values[...], pair[1], cross[1]], axis=0)
    rows = head_rows(queries[...], tiles, heads)
    grads = head_rows(out_grad, tiles, heads)
    mixed = head_rows((out_grad.astype(f32) * attended[...].astype(f32)), tiles, heads)
    delta = lane_total(mixed)
    weight = weights[...]
    grad_scores = dot(grads, bank_v, ((1,), (1,)))
    score_grad = (weight.astype(f32) * (grad_scores - delta) * scale).astype(bf16)
    query_grad[...] = heads_merged(dot(score_grad, bank_k, ((1,), (0,))), tiles, heads).astype(bf16)
    key_all = dot(score_grad, rows, ((0,), (0,)))
    value_all = dot(weight, grads, ((0,), (0,)))
    key_part[...] = key_all[0:own, :]
    value_part[...] = value_all[0:own, :]
    to_pair[0] = key_all[own : own + TILE, :].astype(bf16)
    to_pair[1] = value_all[own : own + TILE, :].astype(bf16)
    to_cross[0] = key_all[own + TILE :, :].astype(bf16)
    to_cross[1] = value_all[own + TILE :, :].astype(bf16)


def combine_kernel(key_part, value_part, from_pair, from_cross, table, key_grad, value_grad):
    tiles = key_part.shape[0] // TILE
    at = tiles * (tiles + 2)
    pair_pick = table[at : at + 1, :]
    cross_pick = table[at + 1 : at + 2, :]
    for k, (part, out) in enumerate(((key_part, key_grad), (value_part, value_grad))):
        for t in range(tiles):
            value = part[t * TILE : (t + 1) * TILE, :]
            value = value + jnp.where(pair_pick == t, from_pair[k].astype(f32), 0.0)
            value = value + jnp.where(cross_pick == t, from_cross[k].astype(f32), 0.0)
            out[t * TILE : (t + 1) * TILE, :] = value.astype(bf16)


def added(parts):
    value = parts[0].astype(f32)
    for j in range(1, parts.shape[0]):
        value = value + parts[j].astype(f32)
    return value.astype(bf16)


def sum_kernel(parts, *rest):
    total = rest[-1]
    value = added(parts)
    for j in range(total.shape[0]):
        total[j] = value


def place_kernel(parts, out, *, scale):
    count, rows_each = parts.shape[0], parts.shape[1]
    column = lax.axis_index("heads")
    share = out.shape[0] // rows_each
    for q in range(count):
        start = pl.multiple_of((column ^ (q // share)) * LANES, LANES)
        row = q % share * rows_each
        out[row : row + rows_each, pl.ds(start, LANES)] = parts[q].astype(f32) * scale


def call(kernel, out_shapes, inputs, name, after=()):
    return pl.pallas_call(
        kernel,
        out_shape=tuple(out_shapes),
        in_specs=vmem(len(inputs)) + [pl.BlockSpec(memory_space=pl.ANY)] * len(after),
        out_specs=tuple(vmem(len(out_shapes))),
        name=name,
    )(*inputs, *after)


def near(array):
    return pltpu.with_memory_space_constraint(array, pltpu.VMEM)


def shape(dims, kind):
    return pltpu.VMEM(tuple(dims), kind)


def final(dims, kind):
    return jax.ShapeDtypeStruct(tuple(dims), kind)


def swapped_heads(value, distance):
    return lax.ppermute(value, "heads", [(i, i ^ distance) for i in range(lax.axis_size("heads"))])


def swapped_pair(value):
    return lax.ppermute(value, "sub", [(0, 1), (1, 0)])


def swapped_cross(value):
    shards = lax.axis_size(NODE_AXES)
    swaps = [(s, s + 1) for s in range(1, shards - 1, 2)]
    return lax.ppermute(value, NODE_AXES, swaps + [(b, a) for a, b in swaps])


def on_device(queries, key_vectors, value_vectors, cotangent, out_weight, neighbours, entry_mask, live_counts, tile_slot):
    row_count, width = queries.shape
    tiles = row_count // TILE
    heads = width // HD
    banks = tiles + 2
    columns = lax.axis_size("heads")
    block = lax.axis_size(BLOCK_AXES)
    others = [swapped_heads(cotangent, k) for k in range(1, columns)]
    table_rows = tiles * banks + 2
    table_rows += -table_rows % 8
    side = shape((2, TILE, width), bf16)
    to_pair, to_cross, table = call(
        select_kernel,
        [side, side, shape((table_rows, LANES), f32)],
        [neighbours.T, entry_mask.T, tile_slot[None, :], live_counts[None, :], key_vectors, value_vectors],
        "select_tiles",
    )
    pair = swapped_pair(to_pair)
    cross = swapped_cross(to_cross)
    stacked = tiles * heads * TILE
    rows_each = columns * width // block
    attended, weights, product = call(
        functools.partial(forward_kernel, heads=heads),
        [shape((row_count, width), bf16), shape((stacked, banks * TILE), bf16), shape((block, rows_each, LANES), bf16)],
        [queries, key_vectors, value_vectors, *map(near, (pair, cross, table)), cotangent, *map(near, others)],
        "attend",
    )
    parts = lax.all_to_all(product, BLOCK_AXES, 0, 0)
    far = lax.axis_size("far")
    (own,) = call(sum_kernel, [shape((far, rows_each, LANES), bf16)], [near(parts)], "sum_block")
    parts = lax.all_to_all(own, "far", 0, 0)
    attended, weights, _ = lax.optimization_barrier((attended, weights, own))
    query_grad, key_part, value_part, pair_part, cross_part = call(
        functools.partial(backward_kernel, heads=heads),
        [final((row_count, width), bf16), shape((row_count, width), f32), shape((row_count, width), f32), side, side],
        [queries, key_vectors, value_vectors, *map(near, (pair, cross, weights, attended)), out_weight, cotangent, *map(near, others)],
        "attend_grad",
    )
    from_cross = swapped_cross(cross_part)
    from_pair = swapped_pair(pair_part)
    key_grad, value_grad = call(
        combine_kernel,
        [final((row_count, width), bf16)] * 2,
        [near(x) for x in (key_part, value_part, from_pair, from_cross, table)],
        "combine",
    )
    (spread,) = call(sum_kernel, [shape((block, rows_each, LANES), bf16)], [near(parts)], "sum_far", (query_grad, key_grad))
    parts = lax.all_to_all(spread, BLOCK_AXES, 0, 0)
    scale = (row_count * lax.axis_size(NODE_AXES)) ** -0.5
    (weight_grad,) = call(
        functools.partial(place_kernel, scale=scale),
        [final((width, columns * LANES), f32)],
        [near(parts)],
        "place",
    )
    return (query_grad, key_grad, value_grad, weight_grad)


def solution(mesh):
    sizes = mesh.shape
    far = sizes["nodes"] // NEAR
    split = jax.sharding.Mesh(
        mesh.devices.reshape(sizes["groups"], far, NEAR, sizes["heads"], sizes["sub"]),
        ("groups", "far", "near", "heads", "sub"),
    )
    rows = P(("groups",) + NODE_AXES, "heads")
    return jax.shard_map(
        on_device,
        mesh=split,
        in_specs=(rows, rows, rows, rows, P("heads", None), P("groups", None), P("groups", None), P("groups"), P("groups")),
        out_specs=(rows, rows, rows, P(("groups", "heads"), None)),
        check_vma=False,
    )
```
